256 devices in a mesh: dp: 16 (over z, x_lo), tensor: 16 (over x_hi, y, core).
Axes of the slice: x: 4 (x_hi: 2, x_lo: 2; x = x_hi * 2 + x_lo), y: 4, z: 8, core: 2. Of those that a mesh axis runs over, the one named last changes fastest.
Arguments:
- hidden_in: bfloat16 [256, 128, 4096], P(('dp', 'tensor')), parts along dimension 0, may hold values from -6 to 6
- norm_gain: float32 [4096], replicated, may hold values from 0.1 to 1.9
- query_weight: bfloat16 [4096, 4096], P(None, 'tensor'), may hold values from -3 to 3
- kv_weight: bfloat16 [4096, 2048], P(None, 'tensor'), may hold values from -3 to 3
- output_weight: bfloat16 [4096, 4096], P('tensor'), may hold values from -0.09375 to 0.09375
Outputs:
- attention_out: bfloat16 [256, 128, 4096], P(('dp', 'tensor')), parts along dimension 0
The draws below stay inside these ranges and needn't reach their ends.
There are 16 independent parts, one for each index of `dp`. The reference program is written for one: setup_inputs(seed, part) draws one part's arguments, and reference() takes and returns one part's arrays. A program takes and returns all parts, laid end to end along the dimension named above; an argument that names none is the same for every part. Nothing has to cross between parts.
All inputs are finite; a program needn't handle non-finite values.
Results may differ from the reference program's by a relative error of at most 0.014.
The reference program's roundings to bfloat16 on the way (of `normed`, `probabilities` and `mixed`) count: a program that leaves them out, or rounds other values in their place, can miss the bound.
Values may be sent and summed in bfloat16 or wider, within the bound.
A program may use at most 128 MiB of HBM per device.

```python
import math
import jax
import jax.numpy as jnp
from jax import lax

D = 4096
H = 32
KVH = 8
HD = 128
SEQ_LEN = 128
SEQS = 16


def projection_base(key):
    base = jnp.clip(jax.random.normal(jax.random.fold_in(key, 11), (D, H * HD), jnp.float32), -4.0, 4.0)
    return base


def draw_query_weight(key, part):
    base = projection_base(key)
    return (base * D ** (-0.5)).astype(jnp.bfloat16)


def draw_kv_weight(key, part):
    own_part = jnp.clip(jax.random.normal(jax.random.fold_in(key, 13), (D, KVH * HD), jnp.float32), -4.0, 4.0)
    value_part = jnp.clip(jax.random.normal(jax.random.fold_in(key, 14), (D, KVH * HD), jnp.float32), -4.0, 4.0)
    key_part = own_part
    joined = jnp.stack((key_part.reshape(D, KVH, HD), value_part.reshape(D, KVH, HD)), axis=2)
    return (joined.reshape(D, 2 * KVH * HD) * D ** (-0.5)).astype(jnp.bfloat16)


def block_levels(key, shape, cuts, smallest, largest):
    gain = 1.0
    for axis_at, blocks in cuts:
        heights = jax.random.uniform(jax.random.fold_in(jax.random.fold_in(key, 6), axis_at), (blocks,), jnp.float32, smallest / len(cuts), largest / len(cuts))
        gain = gain * jnp.repeat(jnp.exp(heights), shape[axis_at] // blocks).reshape((-1,) + (1,) * (len(shape) - 1 - axis_at))
    return gain


def noise(rng, dims, spread, most, shards=(), held_as=jnp.bfloat16):
    values = spread * jax.random.normal(rng, dims, jnp.float32)
    if shards:
        values = values * block_levels(rng, dims, shards, -0.22, 0.18)
    return jnp.clip(values, -most, most).astype(held_as)


def setup_inputs(seed: int = 0, part: int = 0) -> dict:
    seeds = jax.random.split(jax.random.key(seed), 6)
    own_keys = jax.random.split(jax.random.fold_in(seeds[5], part), 6)
    hidden_in = noise(own_keys[0], (SEQS, SEQ_LEN, D), 1.0, 6.0, ((0, 16),))
    norm_gain = jnp.clip(1.0 + 0.18 * jax.random.normal(seeds[1], (D,), jnp.float32), 0.1, 1.9)
    query_weight = draw_query_weight(jax.random.fold_in(seeds[5], 71), part)
    kv_weight = draw_kv_weight(jax.random.fold_in(seeds[5], 71), part)
    output_weight = noise(seeds[4], (H * HD, D), (H * HD) ** -0.5, 0.09375, ((0, 16),))
    return {"hidden_in": hidden_in, "norm_gain": norm_gain, "query_weight": query_weight, "kv_weight": kv_weight, "output_weight": output_weight}


EPS = 1e-05
THETA = 500000.0

def rotary(tensor, positions):
    half_width = tensor.shape[-1] // 2
    frequency = THETA ** (-(jnp.arange(half_width, dtype=jnp.float32) * 2.0 / tensor.shape[-1]))
    angles = positions[:, None] * frequency[None, :]
    cosine = jnp.cos(angles)[:, None, :]
    sine_part = jnp.sin(angles)[:, None, :]
    first_half = tensor[..., :half_width]
    second_half = tensor[..., half_width:]
    return jnp.concatenate((first_half * cosine - second_half * sine_part, second_half * cosine + first_half * sine_part), axis=-1)

def rms_norm(hidden_in, norm_gain):
    wide = hidden_in.astype(jnp.float32)
    mean_square = lax.optimization_barrier(jnp.mean(wide * wide, axis=-1, keepdims=True))
    return (wide * lax.rsqrt(mean_square + EPS) * norm_gain).astype(jnp.bfloat16)

def attend(queries, keys, values):
    length = queries.shape[1]
    scores = jnp.einsum('bqhgd,bkhd->bhgqk', queries.astype(jnp.float32), keys.astype(jnp.float32)) / math.sqrt(queries.shape[-1])
    causal = jnp.arange(length)[:, None] >= jnp.arange(length)[None, :]
    scores = jnp.where(causal, scores, -1e+30)
    highest = lax.optimization_barrier(jnp.max(scores, axis=-1, keepdims=True))
    exponent = jnp.exp(scores - highest)
    probabilities = (exponent / lax.optimization_barrier(jnp.sum(exponent, axis=-1, keepdims=True))).astype(jnp.bfloat16)
    mixed = jnp.einsum('bhgqk,bkhd->bqhgd', probabilities.astype(jnp.float32), values.astype(jnp.float32))
    return mixed.astype(jnp.bfloat16)

def reference(hidden_in, norm_gain, query_weight, kv_weight, output_weight):
    normed = rms_norm(hidden_in, norm_gain).astype(jnp.float32)
    queries_raw = jnp.einsum('bld,dc->blc', normed, query_weight.astype(jnp.float32))
    kv_raw = jnp.einsum('bld,dc->blc', normed, kv_weight.astype(jnp.float32)).astype(jnp.bfloat16)
    kv_split = kv_raw.reshape(SEQS, SEQ_LEN, KVH, 2, HD)
    keys_raw = kv_split[:, :, :, 0, :]
    values = kv_split[:, :, :, 1, :]
    positions = jnp.arange(SEQ_LEN, dtype=jnp.float32)
    queries = rotary(queries_raw.reshape(SEQS, SEQ_LEN, H, HD), positions).astype(jnp.bfloat16)
    keys_wide = lax.optimization_barrier(keys_raw).astype(jnp.float32)
    keys = rotary(keys_wide, positions).astype(jnp.bfloat16)
    mixed = attend(queries.reshape(SEQS, SEQ_LEN, KVH, H // KVH, HD), keys, values)
    result = jnp.einsum('blc,cd->bld', mixed.reshape(SEQS, SEQ_LEN, H * HD).astype(jnp.float32), output_weight.astype(jnp.float32))
    return result.astype(jnp.bfloat16)
```

```python
import math

import jax
import jax.numpy as jnp
import numpy as np
from jax import lax
from jax.experimental import pallas as pl
from jax.experimental.pallas import tpu as pltpu
from jax.sharding import PartitionSpec as P

HD = 128
EPS = 1e-05
THETA = 500000.0
SEQ = 128
D = 4096
HALF = SEQ // 2
RC = 16
NCH = HALF // RC
NS = 4
STEPS = 2 * NS
BF = jnp.bfloat16
F32 = jnp.float32
MESH = pl.DeviceIdType.MESH


def tables():
    i = np.arange(HD // 2, dtype=np.float64)
    ang = np.arange(SEQ, dtype=np.float64)[:, None] * THETA ** (-2.0 * i / HD)[None, :]
    cos, sin = np.cos(ang), np.sin(ang)
    return np.stack(
        [np.concatenate([cos, cos], 1), np.concatenate([-sin, sin], 1)]
    ).astype(np.float32)


def kernel(
    h, gain, tab, wq, wkv, wo, out,
    hbuf, xn, gain_v, tab_v, wq_v, wkv_v, wo_v, mx,
    acc, comb, sbuf, rd, rf, ob,
    sem_l, sem_o, ag_s, ag_r, w_s, w_r, po_s, po_r, rs_s, rs_r,
):
    dp = lax.axis_index("dp")
    t = lax.axis_index("tensor")
    z, xl = dp // 2, dp % 2
    xh, y, c = t // 8, (t // 2) % 4, t % 2
    b = z % 2

    def at_y(yy):
        return (dp, xh * 8 + yy * 2 + c)

    right, left = at_y((y + 1) % 4), at_y((y + 3) % 4)
    cross = (z * 2 + 1 - xl, (1 - xh) * 8 + y * 2 + c)
    xlo = (z * 2 + 1 - xl, t)
    zp = (((z + 1) % 8) * 2 + xl, t)
    zm = (((z + 7) % 8) * 2 + xl, t)
    part = (dp, t + 1 - 2 * c)

    def remote(src, dst, ss, rs, dev):
        return pltpu.make_async_remote_copy(
            src_ref=src, dst_ref=dst, send_sem=ss, recv_sem=rs,
            device_id=dev, device_id_type=MESH,
        )

    loads = [
        pltpu.make_async_copy(h.at[0], hbuf.at[0], sem_l.at[0]),
        pltpu.make_async_copy(gain, gain_v, sem_l.at[1]),
        pltpu.make_async_copy(tab, tab_v, sem_l.at[2]),
        pltpu.make_async_copy(wq, wq_v.at[0, c], sem_l.at[3]),
        pltpu.make_async_copy(
            wkv, wkv_v.at[0, :, pl.ds(pl.multiple_of(c * HD, HD), HD)], sem_l.at[4]
        ),
        pltpu.make_async_copy(wo, wo_v.at[0, c], sem_l.at[5]),
    ]
    for cp in loads:
        cp.start()

    barrier = pltpu.get_barrier_semaphore()
    for dev in (right, left, cross, xlo, zp, zm, part):
        pl.semaphore_signal(barrier, inc=1, device_id=dev, device_id_type=MESH)
    pl.semaphore_wait(barrier, 7)

    sent = []

    def go(cp):
        cp.start()
        sent.append(cp)

    def rows(ref, half):
        return ref.at[pl.ds(half * HALF, HALF), :]

    def ag_own(direction, half):
        dst = hbuf.at[1 if direction == 0 else 2]
        return remote(
            rows(h.at[0], half), rows(dst, half),
            ag_s.at[direction, half], ag_r.at[1 + direction, half],
            right if direction == 0 else left,
        )

    def ag_fwd(direction):
        half = direction
        return remote(
            rows(hbuf.at[1 + direction], half), rows(hbuf.at[3], half),
            ag_s.at[direction, 2], ag_r.at[3, half],
            right if direction == 0 else left,
        )

    def ag_wait(slot, half):
        remote(
            rows(hbuf.at[slot], half), rows(hbuf.at[slot], half),
            ag_s.at[0, 0], ag_r.at[slot, half], right,
        ).wait_recv()

    go(ag_own(0, 0))
    go(ag_own(1, 1))
    go(ag_own(0, 1))
    go(ag_own(1, 0))

    def region(m, g, core, q, i):
        if m == 0:
            return wq_v.at[g, core, pl.ds(q * 1024 + i * 256, 256), :]
        if m == 1:
            return wkv_v.at[
                g, pl.ds(q * 1024 + i * 256, 256),
                pl.ds(pl.multiple_of(core * HD, HD), HD),
            ]
        return wo_v.at[g, core, pl.ds(q * 64 + i * 16, 16), :]

    def own_region(m, q, i):
        if m == 0:
            return wq.at[pl.ds(q * 1024 + i * 256, 256), :]
        if m == 1:
            return wkv.at[pl.ds(q * 1024 + i * 256, 256), :]
        return wo.at[pl.ds(q * 64 + i * 16, 16), :]

    def parts(s):
        return [(0, s), (1, s)] if s < NS else [(2, s - NS)]

    def sem_ix(m, i):
        return m * NS + i

    q_cc = 2 * xl + b
    q_x = 2 * (1 - xl) + b
    q_zc = 2 * xl + 1 - b
    q_zx = 2 * (1 - xl) + 1 - b

    def cross_send(s):
        for m, i in parts(s):
            q = 2 * (1 - xl) + b
            k = sem_ix(m, i)
            go(remote(own_region(m, q, i), region(m, 1, c, q, i),
                      w_s.at[0, k], w_r.at[0, k], cross))

    def w_wait(ch, m, core, q, i):
        k = sem_ix(m, i)
        reg = region(m, 1, core, q, i)
        remote(reg, reg, w_s.at[ch, k], w_r.at[ch, k], part).wait_recv()

    def w_send(ch, m, q, i, dev):
        k = sem_ix(m, i)
        reg = region(m, 1, c, q, i)
        go(remote(reg, reg, w_s.at[ch, k], w_r.at[ch, k], dev))

    def z_dev(i):
        return zp if i % 2 == 0 else zm

    def relay(T):
        if 0 <= T < STEPS:
            for m, i in parts(T):
                w_wait(0, m, c, q_cc, i)
                w_send(1, m, q_cc, i, xlo)
                w_send(2, m, q_cc, i, z_dev(i))
                w_send(4, m, q_cc, i, part)
        if 0 <= T - 1 < STEPS:
            for m, i in parts(T - 1):
                w_wait(1, m, c, q_x, i)
                w_send(3, m, q_x, i, z_dev(i))
                w_send(5, m, q_x, i, part)
            for m, i in parts(T - 1):
                w_wait(2, m, c, q_zc, i)
                w_send(6, m, q_zc, i, part)
        if 0 <= T - 2 < STEPS:
            for m, i in parts(T - 2):
                w_wait(3, m, c, q_zx, i)
                w_send(7, m, q_zx, i, part)

    def part_wait(m):
        for i in range(NS):
            for ch, q in ((4, q_cc), (5, q_x), (6, q_zc), (7, q_zx)):
                w_wait(ch, m, 1 - c, q, i)

    def own_to_part(m):
        src = (wq, wkv, wo)[m]
        dst = (
            wq_v.at[0, c],
            wkv_v.at[0, :, pl.ds(pl.multiple_of(c * HD, HD), HD)],
            wo_v.at[0, c],
        )[m]
        return remote(src, dst, po_s.at[m], po_r.at[m], part)

    def own_part_wait(m):
        dst = (
            wq_v.at[0, 1 - c],
            wkv_v.at[0, :, pl.ds(pl.multiple_of((1 - c) * HD, HD), HD)],
            wo_v.at[0, 1 - c],
        )[m]
        remote(dst, dst, po_s.at[m], po_r.at[m], part).wait_recv()

    for s in range(STEPS):
        cross_send(s)
    for m in range(3):
        go(own_to_part(m))

    def norm(slot):
        @pl.loop(0, SEQ // 16)
        def _(r):
            r0 = pl.multiple_of(r * 16, 16)
            wide = hbuf[slot, pl.ds(r0, 16), :].astype(F32)
            ms = jnp.mean(wide * wide, axis=-1, keepdims=True)
            xn[slot, pl.ds(r0, 16), :] = (
                wide * lax.rsqrt(ms + EPS) * gain_v[...]
            ).astype(BF)

    def rope(v):
        return v * tab_v[0] + pltpu.roll(v, HD // 2, 1) * tab_v[1]

    def attn(slot, g):
        x = xn[slot]
        kv = jnp.dot(x, wkv_v[g], preferred_element_type=F32).astype(BF)
        q0 = jnp.dot(x, wq_v[g, 0], preferred_element_type=F32)
        q1 = jnp.dot(x, wq_v[g, 1], preferred_element_type=F32)
        keys = rope(kv[:, :HD].astype(F32)).astype(BF)
        vals = kv[:, HD:]
        qs = jnp.concatenate(
            [rope(v).astype(BF) for v in (q0[:, :HD], q0[:, HD:], q1[:, :HD], q1[:, HD:])],
            axis=0,
        )
        sc = lax.dot_general(
            qs, keys, (((1,), (1,)), ((), ())), preferred_element_type=F32
        ) * (1.0 / math.sqrt(HD))
        rowi = lax.broadcasted_iota(jnp.int32, sc.shape, 0) % SEQ
        coli = lax.broadcasted_iota(jnp.int32, sc.shape, 1)
        sc = jnp.where(rowi >= coli, sc, -1e30)
        e = jnp.exp(sc - jnp.max(sc, axis=-1, keepdims=True))
        p = (e / jnp.sum(e, axis=-1, keepdims=True)).astype(BF)
        o = jnp.dot(p, vals, preferred_element_type=F32).astype(BF)
        for j in range(4):
            mx[slot, :, pl.ds(g * 512 + j * HD, HD)] = o[j * SEQ:(j + 1) * SEQ]

    NB = 512

    def outp(slot):
        @pl.loop(0, D // NB)
        def _(n):
            cols = pl.ds(pl.multiple_of(n * NB, NB), NB)
            o = jnp.zeros((SEQ, NB), F32)
            for k in range(4):
                o = o + jnp.dot(
                    mx[slot, :, pl.ds(k * 256, 256)], wo_v[k // 2, k % 2, :, cols],
                    preferred_element_type=F32,
                )
            if slot == 0:
                acc[:, cols] = o
            elif slot == 1:
                sbuf[0, pl.ds(0, HALF), cols] = o[:HALF].astype(BF)
                comb[1, :, cols] = o[HALF:]
            elif slot == 2:
                sbuf[1, pl.ds(HALF, HALF), cols] = o[HALF:].astype(BF)
                comb[0, :, cols] = o[:HALF]
            else:
                sbuf[2, :, cols] = o.astype(BF)

    def rc(ref, half, r):
        return ref.at[pl.ds(half * HALF + r * RC, RC), :]

    def rs_only(direction):
        half = 1 - direction
        src = sbuf.at[1 - direction]
        return remote(rows(src, half), rows(rf.at[direction], half),
                      rs_s.at[direction, 0], rs_r.at[direction, 0],
                      right if direction == 0 else left)

    def rs_diag(direction, r):
        return remote(rc(sbuf.at[2], direction, r),
                      rd.at[direction, pl.ds(r * RC, RC), :],
                      rs_s.at[direction, 1 + r], rs_r.at[direction, 1 + r],
                      right if direction == 0 else left)

    def rs_comb(direction, r):
        k = 1 + NCH + r
        return remote(rc(sbuf.at[1 - direction], direction, r),
                      rc(rf.at[direction], direction, r),
                      rs_s.at[direction, k], rs_r.at[direction, k],
                      right if direction == 0 else left)

    loads[0].wait()
    loads[1].wait()
    norm(0)
    relay(0)
    relay(1)
    for cp in loads[2:5]:
        cp.wait()
    own_part_wait(0)
    own_part_wait(1)
    attn(0, 0)
    ag_wait(1, 0)
    ag_wait(2, 1)
    go(ag_fwd(0))
    go(ag_fwd(1))
    relay(2)
    relay(3)
    relay(4)
    ag_wait(1, 1)
    norm(1)
    ag_wait(2, 0)
    norm(2)
    attn(1, 0)
    relay(5)
    attn(2, 0)
    part_wait(0)
    part_wait(1)
    attn(0, 1)
    relay(6)
    attn(1, 1)
    relay(7)
    attn(2, 1)
    relay(8)
    ag_wait(3, 0)
    ag_wait(3, 1)
    norm(3)
    attn(3, 0)
    relay(9)
    loads[5].wait()
    own_part_wait(2)
    part_wait(2)
    outp(2)
    go(rs_only(0))
    outp(1)
    go(rs_only(1))
    attn(3, 1)
    outp(3)
    for r in range(NCH):
        go(rs_diag(0, r))
        go(rs_diag(1, r))
    outp(0)
    for r in range(NCH):
        for direction in (0, 1):
            rs_diag(direction, r).wait_recv()
            rr = pl.ds(r * RC, RC)
            v = comb[direction, rr, :] + rd[direction, rr, :].astype(F32)
            sbuf[1 - direction, pl.ds(direction * HALF + r * RC, RC), :] = v.astype(BF)
            go(rs_comb(direction, r))
    rs_only(0).wait_recv()
    rs_only(1).wait_recv()
    outs = []
    for r in range(NCH):
        for half in (0, 1):
            rs_comb(half, r).wait_recv()
            rr = pl.ds(half * HALF + r * RC, RC)
            v = acc[rr, :] + rf[0, rr, :].astype(F32) + rf[1, rr, :].astype(F32)
            ob[rr, :] = v.astype(BF)
            cp = pltpu.make_async_copy(
                ob.at[rr, :], out.at[0, rr, :], sem_o.at[half, r]
            )
            cp.start()
            outs.append(cp)
    for cp in outs:
        cp.wait()
    for cp in sent:
        cp.wait_send()


def shards(hidden_in, norm_gain, query_weight, kv_weight, output_weight):
    tab = jnp.asarray(tables())
    anyspec = pl.BlockSpec(memory_space=pl.ANY)
    dma = pltpu.SemaphoreType.DMA
    return pl.pallas_call(
        kernel,
        out_shape=jax.ShapeDtypeStruct((1, SEQ, D), BF),
        in_specs=[anyspec] * 6,
        out_specs=anyspec,
        scratch_shapes=[
            pltpu.VMEM((4, SEQ, D), BF),
            pltpu.VMEM((4, SEQ, D), BF),
            pltpu.VMEM((1, D), F32),
            pltpu.VMEM((2, SEQ, HD), F32),
            pltpu.VMEM((2, 2, D, 2 * HD), BF),
            pltpu.VMEM((2, D, 2 * HD), BF),
            pltpu.VMEM((2, 2, 2 * HD, D), BF),
            pltpu.VMEM((4, SEQ, 1024), BF),
            pltpu.VMEM((SEQ, D), F32),
            pltpu.VMEM((2, HALF, D), F32),
            pltpu.VMEM((3, SEQ, D), BF),
            pltpu.VMEM((2, HALF, D), BF),
            pltpu.VMEM((2, SEQ, D), BF),
            pltpu.VMEM((SEQ, D), BF),
            dma((6,)),
            dma((2, NCH)),
            dma((2, 3)),
            dma((4, 2)),
            dma((8, 3 * NS)),
            dma((8, 3 * NS)),
            dma((3,)),
            dma((3,)),
            dma((2, 1 + 2 * NCH)),
            dma((2, 1 + 2 * NCH)),
        ],
        compiler_params=pltpu.CompilerParams(
            collective_id=0, has_side_effects=True, vmem_limit_bytes=67000000
        ),
        cost_estimate=pl.CostEstimate(
            flops=11_000_000_000, bytes_accessed=8_000_000, transcendentals=600_000
        ),
    )(hidden_in, norm_gain.reshape(1, D), tab, query_weight, kv_weight, output_weight)


def solution(mesh):
    placed = (
        P(("dp", "tensor"), None, None),
        P(),
        P(None, "tensor"),
        P(None, "tensor"),
        P("tensor", None),
    )
    return jax.shard_map(
        shards,
        mesh=mesh,
        in_specs=placed,
        out_specs=P(("dp", "tensor"), None, None),
        check_vma=False,
    )
```

```python
import math

import jax
import jax.numpy as jnp
import numpy as np
from jax import lax
from jax.experimental import pallas as pl
from jax.experimental.pallas import tpu as pltpu
from jax.sharding import PartitionSpec as P

HD = 128
EPS = 1e-05
THETA = 500000.0
SEQ = 128
D = 4096
HALF = SEQ // 2
CW = 1024
NC = D // CW
NQ = 8
NSTEP = NQ + NC
BF = jnp.bfloat16
F32 = jnp.float32
MESH = pl.DeviceIdType.MESH


def tables():
    i = np.arange(HD // 2, dtype=np.float64)
    ang = np.arange(SEQ, dtype=np.float64)[:, None] * THETA ** (-2.0 * i / HD)[None, :]
    cos, sin = np.cos(ang), np.sin(ang)
    return np.stack(
        [np.concatenate([cos, cos], 1), np.concatenate([-sin, sin], 1)]
    ).astype(np.float32)


def kernel(
    h, gain, tab, wq, wkv, wo, out,
    hbuf, xn, gain_v, tab_v, wq_v, wkv_v, wo_v, mx,
    acc, comb, sbuf, rd, rf, ob,
    sem_l, sem_o, ag_s, ag_r, w_s, w_r, po_s, po_r, rs_s, rs_r,
):
    dp = lax.axis_index("dp")
    t = lax.axis_index("tensor")
    z, xl = dp // 2, dp % 2
    xh, y, c = t // 8, (t // 2) % 4, t % 2
    b = z % 2

    def at_y(yy):
        return (dp, xh * 8 + yy * 2 + c)

    right, left = at_y((y + 1) % 4), at_y((y + 3) % 4)
    cross = (z * 2 + 1 - xl, (1 - xh) * 8 + y * 2 + c)
    xlo = (z * 2 + 1 - xl, t)
    zp = (((z + 1) % 8) * 2 + xl, t)
    zm = (((z + 7) % 8) * 2 + xl, t)
    part = (dp, t + 1 - 2 * c)

    def remote(src, dst, ss, rs, dev):
        return pltpu.make_async_remote_copy(
            src_ref=src, dst_ref=dst, send_sem=ss, recv_sem=rs,
            device_id=dev, device_id_type=MESH,
        )

    loads = [
        pltpu.make_async_copy(h.at[0], hbuf.at[0], sem_l.at[0]),
        pltpu.make_async_copy(gain, gain_v, sem_l.at[1]),
        pltpu.make_async_copy(tab, tab_v, sem_l.at[2]),
        pltpu.make_async_copy(wq, wq_v.at[0, c], sem_l.at[3]),
        pltpu.make_async_copy(
            wkv, wkv_v.at[0, :, pl.ds(pl.multiple_of(c * HD, HD), HD)], sem_l.at[4]
        ),
        pltpu.make_async_copy(
            wo, wo_v.at[pl.ds(pl.multiple_of(c * 256, 256), 256), :], sem_l.at[5]
        ),
    ]
    for cp in loads:
        cp.start()

    barrier = pltpu.get_barrier_semaphore()
    for dev in (right, left, cross, xlo, zp, zm, part):
        pl.semaphore_signal(barrier, inc=1, device_id=dev, device_id_type=MESH)
    pl.semaphore_wait(barrier, 7)

    sent = []

    def go(cp):
        cp.start()
        sent.append(cp)

    def rows(ref, half):
        return ref.at[pl.ds(half * HALF, HALF), :]

    def ag_own(direction, half):
        dst = hbuf.at[1 if direction == 0 else 2]
        return remote(
            rows(h.at[0], half), rows(dst, half),
            ag_s.at[direction, half], ag_r.at[1 + direction, half],
            right if direction == 0 else left,
        )

    def ag_fwd(direction):
        half = direction
        return remote(
            rows(hbuf.at[1 + direction], half), rows(hbuf.at[3], half),
            ag_s.at[direction, 2], ag_r.at[3, half],
            right if direction == 0 else left,
        )

    def ag_wait(slot, half):
        remote(
            rows(hbuf.at[slot], half), rows(hbuf.at[slot], half),
            ag_s.at[0, 0], ag_r.at[slot, half], right,
        ).wait_recv()

    go(ag_own(0, 0))
    go(ag_own(1, 1))
    go(ag_own(0, 1))
    go(ag_own(1, 0))

    QR = D // 4 // NQ

    def region(m, g, core, q, i):
        r = pl.ds(pl.multiple_of(q * (D // 4) + i * QR, QR), QR)
        if m == 0:
            return wq_v.at[g, core, r, :]
        if m == 1:
            return wkv_v.at[g, r, pl.ds(pl.multiple_of(core * HD, HD), HD)]
        return wo_v.at[
            pl.ds(pl.multiple_of((g * 2 + core) * 256, 256), 256),
            pl.ds(pl.multiple_of(i * CW + q * 256, 256), 256),
        ]

    def own_region(m, q, i):
        r = pl.ds(pl.multiple_of(q * (D // 4) + i * QR, QR), QR)
        if m == 0:
            return wq.at[r, :]
        if m == 1:
            return wkv.at[r, :]
        return wo.at[:, pl.ds(pl.multiple_of(i * CW + q * 256, 256), 256)]

    def parts(s):
        return [(0, s), (1, s)] if s < NQ else [(2, s - NQ)]

    def sem_ix(m, i):
        return m * NQ + i

    q_cc = 2 * xl + b
    q_x = 2 * (1 - xl) + b
    q_zc = 2 * xl + 1 - b
    q_zx = 2 * (1 - xl) + 1 - b

    def cross_send(s):
        for m, i in parts(s):
            k = sem_ix(m, i)
            go(remote(own_region(m, q_x, i), region(m, 1, c, q_x, i),
                      w_s.at[0, k], w_r.at[0, k], cross))

    def w_wait(ch, m, core, q, i):
        k = sem_ix(m, i)
        reg = region(m, 1, core, q, i)
        remote(reg, reg, w_s.at[ch, k], w_r.at[ch, k], part).wait_recv()

    def w_send(ch, m, q, i, dev):
        k = sem_ix(m, i)
        reg = region(m, 1, c, q, i)
        go(remote(reg, reg, w_s.at[ch, k], w_r.at[ch, k], dev))

    def ev_cross(s):
        z_dev = zp if s % 2 == 0 else zm
        for m, i in parts(s):
            w_wait(0, m, c, q_cc, i)
            w_send(1, m, q_cc, i, xlo)
            w_send(2, m, q_cc, i, z_dev)
            w_send(4, m, q_cc, i, part)

    def ev_xlo(s):
        z_dev = zp if s % 2 == 0 else zm
        for m, i in parts(s):
            w_wait(1, m, c, q_x, i)
            w_send(3, m, q_x, i, z_dev)
            w_send(5, m, q_x, i, part)

    def ev_zc(s):
        for m, i in parts(s):
            w_wait(2, m, c, q_zc, i)
            w_send(6, m, q_zc, i, part)

    def ev_zx(s):
        for m, i in parts(s):
            w_wait(3, m, c, q_zx, i)
            w_send(7, m, q_zx, i, part)

    def part_wait(steps):
        for s in steps:
            for m, i in parts(s):
                for ch, q in ((4, q_cc), (5, q_x), (6, q_zc), (7, q_zx)):
                    w_wait(ch, m, 1 - c, q, i)

    def own_dst(m, core):
        return (
            wq_v.at[0, core],
            wkv_v.at[0, :, pl.ds(pl.multiple_of(core * HD, HD), HD)],
            wo_v.at[pl.ds(pl.multiple_of(core * 256, 256), 256), :],
        )[m]

    def own_to_part(m):
        go(remote((wq, wkv, wo)[m], own_dst(m, c), po_s.at[m], po_r.at[m], part))

    def own_part_wait(m):
        dst = own_dst(m, 1 - c)
        remote(dst, dst, po_s.at[m], po_r.at[m], part).wait_recv()

    def norm(slot, half):
        @pl.loop(0, HALF // 16)
        def _(r):
            r0 = pl.multiple_of(half * HALF + r * 16, 16)
            wide = hbuf[slot, pl.ds(r0, 16), :].astype(F32)
            ms = jnp.mean(wide * wide, axis=-1, keepdims=True)
            xn[slot, pl.ds(r0, 16), :] = (
                wide * lax.rsqrt(ms + EPS) * gain_v[...]
            ).astype(BF)

    def rope(v):
        return v * tab_v[0] + pltpu.roll(v, HD // 2, 1) * tab_v[1]

    def attn(slot, g):
        x = xn[slot]
        kv = jnp.dot(x, wkv_v[g], preferred_element_type=F32).astype(BF)
        q0 = jnp.dot(x, wq_v[g, 0], preferred_element_type=F32)
        q1 = jnp.dot(x, wq_v[g, 1], preferred_element_type=F32)
        keys = rope(kv[:, :HD].astype(F32)).astype(BF)
        vals = kv[:, HD:]
        qs = jnp.concatenate(
            [rope(v).astype(BF) for v in (q0[:, :HD], q0[:, HD:], q1[:, :HD], q1[:, HD:])],
            axis=0,
        )
        sc = lax.dot_general(
            qs, keys, (((1,), (1,)), ((), ())), preferred_element_type=F32
        ) * (1.0 / math.sqrt(HD))
        rowi = lax.broadcasted_iota(jnp.int32, sc.shape, 0) % SEQ
        coli = lax.broadcasted_iota(jnp.int32, sc.shape, 1)
        sc = jnp.where(rowi >= coli, sc, -1e30)
        e = jnp.exp(sc - jnp.max(sc, axis=-1, keepdims=True))
        p = (e / jnp.sum(e, axis=-1, keepdims=True)).astype(BF)
        o = jnp.dot(p, vals, preferred_element_type=F32).astype(BF)
        for j in range(4):
            mx[slot, :, pl.ds(g * 512 + j * HD, HD)] = o[j * SEQ:(j + 1) * SEQ]

    def outp(slot, i):
        cols = pl.ds(i * CW, CW)
        o = jnp.dot(mx[slot], wo_v[:, cols], preferred_element_type=F32)
        if slot == 0:
            acc[:, cols] = o
        elif slot == 1:
            sbuf[0, pl.ds(0, HALF), cols] = o[:HALF].astype(BF)
            comb[1, :, cols] = o[HALF:]
        elif slot == 2:
            sbuf[1, pl.ds(HALF, HALF), cols] = o[HALF:].astype(BF)
            comb[0, :, cols] = o[:HALF]
        else:
            sbuf[2, :, cols] = o.astype(BF)

    def blk(ref, half, i):
        return ref.at[pl.ds(half * HALF, HALF), pl.ds(i * CW, CW)]

    def y_copy(direction, k, src, dst):
        return remote(src, dst, rs_s.at[direction, k], rs_r.at[direction, k],
                      right if direction == 0 else left)

    def rs_only(d, i):
        return y_copy(d, i, blk(sbuf.at[1 - d], 1 - d, i), blk(rf.at[d], 1 - d, i))

    def rs_diag(d, i):
        return y_copy(d, NC + i, blk(sbuf.at[2], d, i), blk(rd.at[d], 0, i))

    def rs_comb(d, i):
        return y_copy(d, 2 * NC + i, blk(sbuf.at[1 - d], d, i), blk(rf.at[d], d, i))

    def combine(d, i):
        rs_diag(d, i).wait_recv()
        cols = pl.ds(i * CW, CW)
        v = comb[d, :, cols] + rd[d, :, cols].astype(F32)
        sbuf[1 - d, pl.ds(d * HALF, HALF), cols] = v.astype(BF)
        go(rs_comb(d, i))

    outs = []

    def finish(half, i):
        rs_only(1 - half, i).wait_recv()
        rs_comb(half, i).wait_recv()
        rr, cols = pl.ds(half * HALF, HALF), pl.ds(i * CW, CW)
        v = acc[rr, cols] + rf[0, rr, cols].astype(F32) + rf[1, rr, cols].astype(F32)
        ob[rr, cols] = v.astype(BF)
        cp = pltpu.make_async_copy(
            ob.at[rr, cols], out.at[0, rr, cols], sem_o.at[half, i]
        )
        cp.start()
        outs.append(cp)

    plan = []

    def due(time, fn, *args):
        plan.append((time, len(plan), fn, args))

    def loaded(*ks):
        for k in ks:
            loads[k].wait()

    def ag_first():
        ag_wait(1, 0)
        go(ag_fwd(0))
        ag_wait(2, 1)
        go(ag_fwd(1))

    def outp_send(i):
        part_wait([NQ + i])
        outp(2, i)
        go(rs_only(0, i))
        outp(1, i)
        go(rs_only(1, i))

    def outp_diag(i):
        outp(3, i)
        go(rs_diag(0, i))
        go(rs_diag(1, i))

    for s in range(NSTEP):
        tc = 7 + 2.1 * (s + 1) if s < NQ else 7 + 2.1 * NQ + 2.8 * (s - NQ + 1)
        due(tc, ev_cross, s)
        due(tc + 4.1, ev_xlo, s)
        due(tc + 4.1, ev_zc, s)
        due(tc + 8.2, ev_zx, s)
    due(4.5, loaded, 0, 1)
    due(4.5, norm, 0, 0)
    due(4.5, norm, 0, 1)
    due(11.3, loaded, 2, 3, 4)
    due(11.3, own_part_wait, 0)
    due(11.3, own_part_wait, 1)
    due(11.3, attn, 0, 0)
    due(11.4, own_to_part, 2)
    due(18, ag_first)
    due(18, norm, 1, 0)
    due(18, norm, 2, 1)
    due(29.5, ag_wait, 1, 1)
    due(29.5, norm, 1, 1)
    due(29.5, ag_wait, 2, 0)
    due(29.5, norm, 2, 0)
    due(30.5, attn, 2, 0)
    due(32.1, attn, 1, 0)
    due(33.9, part_wait, range(NQ))
    due(33.9, attn, 2, 1)
    due(35.5, attn, 1, 1)
    due(37, loaded, 5)
    due(37, own_part_wait, 2)
    due(37.2, outp_send, 0)
    due(38.5, attn, 0, 1)
    due(40.3, outp_send, 1)
    due(40.8, ag_wait, 3, 0)
    due(40.8, ag_wait, 3, 1)
    due(40.8, norm, 3, 0)
    due(40.8, norm, 3, 1)
    due(42, attn, 3, 0)
    due(43.3, outp_send, 2)
    due(44, attn, 3, 1)
    due(46, outp_send, 3)
    for i in range(NC):
        due(47, outp_diag, i)
    for i in range(NC):
        due(48, outp, 0, i)
    for i in range(NC):
        due(50, combine, 0, i)
        due(50, combine, 1, i)
    for i in range(NC):
        due(60, finish, 0, i)
        due(60, finish, 1, i)

    for s in range(NSTEP):
        cross_send(s)
    own_to_part(0)
    own_to_part(1)
    for time, _, fn, args in sorted(plan, key=lambda p: p[:2]):
        fn(*args)
    for cp in outs:
        cp.wait()
    for cp in sent:
        cp.wait_send()


def shards(hidden_in, norm_gain, query_weight, kv_weight, output_weight):
    tab = jnp.asarray(tables())
    anyspec = pl.BlockSpec(memory_space=pl.ANY)
    dma = pltpu.SemaphoreType.DMA
    return pl.pallas_call(
        kernel,
        out_shape=jax.ShapeDtypeStruct((1, SEQ, D), BF),
        in_specs=[anyspec] * 6,
        out_specs=anyspec,
        scratch_shapes=[
            pltpu.VMEM((4, SEQ, D), BF),
            pltpu.VMEM((4, SEQ, D), BF),
            pltpu.VMEM((1, D), F32),
            pltpu.VMEM((2, SEQ, HD), F32),
            pltpu.VMEM((2, 2, D, 2 * HD), BF),
            pltpu.VMEM((2, D, 2 * HD), BF),
            pltpu.VMEM((1024, D), BF),
            pltpu.VMEM((4, SEQ, 1024), BF),
            pltpu.VMEM((SEQ, D), F32),
            pltpu.VMEM((2, HALF, D), F32),
            pltpu.VMEM((3, SEQ, D), BF),
            pltpu.VMEM((2, HALF, D), BF),
            pltpu.VMEM((2, SEQ, D), BF),
            pltpu.VMEM((SEQ, D), BF),
            dma((6,)),
            dma((2, NC)),
            dma((2, 3)),
            dma((4, 2)),
            dma((8, 2 * NQ + NC)),
            dma((8, 2 * NQ + NC)),
            dma((3,)),
            dma((3,)),
            dma((2, 3 * NC)),
            dma((2, 3 * NC)),
        ],
        compiler_params=pltpu.CompilerParams(
            collective_id=0, has_side_effects=True, vmem_limit_bytes=67000000
        ),
        cost_estimate=pl.CostEstimate(
            flops=11_000_000_000, bytes_accessed=8_000_000, transcendentals=600_000
        ),
    )(hidden_in, norm_gain.reshape(1, D), tab, query_weight, kv_weight, output_weight)


def solution(mesh):
    placed = (
        P(("dp", "tensor"), None, None),
        P(),
        P(None, "tensor"),
        P(None, "tensor"),
        P("tensor", None),
    )
    return jax.shard_map(
        shards,
        mesh=mesh,
        in_specs=placed,
        out_specs=P(("dp", "tensor"), None, None),
        check_vma=False,
    )
```

```python
import math

import jax
import jax.numpy as jnp
import numpy as np
from jax import lax
from jax.experimental import pallas as pl
from jax.experimental.pallas import tpu as pltpu
from jax.sharding import PartitionSpec as P

HD = 128
EPS = 1e-05
THETA = 500000.0
SEQ = 128
D = 4096
HALF = SEQ // 2
QROWS = (80, 80, 96, 128, 128, 96, 80, 80, 96, 96, 64)
QOFF = tuple(sum(QROWS[:i]) for i in range(len(QROWS)))
NQ = len(QROWS)
GROUPS = ((0, 5, 0, 512), (5, 3, 512, 256), (8, 3, 768, 256))
CWS = (512, 512, 1024, 1024, 512, 512)
COFF = tuple(sum(CWS[:i]) for i in range(len(CWS)))
NC = len(CWS)
NSTEP = NQ + NC
DIRECT = NQ + 2
QD = D // 4
BF = jnp.bfloat16
F32 = jnp.float32
MESH = pl.DeviceIdType.MESH


def tables():
    i = np.arange(HD // 2, dtype=np.float64)
    ang = np.arange(SEQ, dtype=np.float64)[:, None] * THETA ** (-2.0 * i / HD)[None, :]
    cos, sin = np.cos(ang), np.sin(ang)
    return np.stack(
        [np.concatenate([cos, cos], 1), np.concatenate([-sin, sin], 1)]
    ).astype(np.float32)


def arrivals(start):
    rate, hop = 46.6e3, 2.0
    size = [2 * r * 3 * HD for r in QROWS] + [2 * 2 * HD * w // 4 for w in CWS]
    wire = [b / rate for b in size]
    t_zc, t_zx = [0.0] * NSTEP, [0.0] * NSTEP
    t_c, free = [], start + 1.0
    for w in wire:
        free += w
        t_c.append(free + hop)
    for s in range(DIRECT, NSTEP):
        free += wire[s]
        t_zx[s] = free + hop
    t_x, free = [], 0.0
    for s, w in enumerate(wire):
        free = max(free, t_c[s]) + w
        t_x.append(free + hop)
    for side in (0, 1):
        jobs = [(t_c[s], 0, s) for s in range(side, NSTEP, 2)]
        jobs += [(t_x[s], 1, s) for s in range(side, DIRECT, 2)]
        free = 0.0
        for ready, kind, s in sorted(jobs):
            free = max(free, ready) + wire[s]
            (t_zc, t_zx)[kind][s] = free + hop
    return t_c, t_x, t_zc, t_zx


def kernel(
    h, gain, tab, wq, wkv, wo, out,
    hbuf, xn, gain_v, tab_v, wq_v, wkv_v, wo_v, mx, pacc,
    acc, comb, sbuf, rd, rf, ob,
    sem_l, sem_o, ag_s, ag_r, w_s, w_r, po_s, po_r, rs_s, rs_r,
):
    dp = lax.axis_index("dp")
    t = lax.axis_index("tensor")
    z, xl = dp // 2, dp % 2
    xh, y, c = t // 8, (t // 2) % 4, t % 2
    b = z % 2

    def at_y(yy):
        return (dp, xh * 8 + yy * 2 + c)

    right, left = at_y((y + 1) % 4), at_y((y + 3) % 4)
    cross = (z * 2 + 1 - xl, (1 - xh) * 8 + y * 2 + c)
    xlo = (z * 2 + 1 - xl, t)
    zp = (((z + 1) % 8) * 2 + xl, t)
    zm = (((z + 7) % 8) * 2 + xl, t)
    part = (dp, t + 1 - 2 * c)

    def remote(src, dst, ss, rs, dev):
        return pltpu.make_async_remote_copy(
            src_ref=src, dst_ref=dst, send_sem=ss, recv_sem=rs,
            device_id=dev, device_id_type=MESH,
        )

    loads = [
        pltpu.make_async_copy(h.at[0], hbuf.at[0], sem_l.at[0]),
        pltpu.make_async_copy(gain, gain_v, sem_l.at[1]),
        pltpu.make_async_copy(tab, tab_v, sem_l.at[2]),
        pltpu.make_async_copy(wq, wq_v.at[0, c], sem_l.at[3]),
        pltpu.make_async_copy(
            wkv, wkv_v.at[0, :, pl.ds(pl.multiple_of(c * HD, HD), HD)], sem_l.at[4]
        ),
        pltpu.make_async_copy(
            wo, wo_v.at[pl.ds(pl.multiple_of(c * 256, 256), 256), :], sem_l.at[5]
        ),
    ]
    for cp in loads:
        cp.start()

    barrier = pltpu.get_barrier_semaphore()
    for dev in (right, left, cross, xlo, zp, zm, part):
        pl.semaphore_signal(barrier, inc=1, device_id=dev, device_id_type=MESH)
    pl.semaphore_wait(barrier, 7)

    sent = []

    def go(cp):
        cp.start()
        sent.append(cp)

    def rows(ref, half):
        return ref.at[pl.ds(half * HALF, HALF), :]

    def ag_own(direction, half):
        dst = hbuf.at[1 if direction == 0 else 2]
        return remote(
            rows(h.at[0], half), rows(dst, half),
            ag_s.at[direction, half], ag_r.at[1 + direction, half],
            right if direction == 0 else left,
        )

    def ag_fwd(direction):
        half = direction
        return remote(
            rows(hbuf.at[1 + direction], half), rows(hbuf.at[3], half),
            ag_s.at[direction, 2], ag_r.at[3, half],
            right if direction == 0 else left,
        )

    def ag_wait(slot, half):
        remote(
            rows(hbuf.at[slot], half), rows(hbuf.at[slot], half),
            ag_s.at[0, 0], ag_r.at[slot, half], right,
        ).wait_recv()

    go(ag_own(0, 0))
    go(ag_own(1, 1))
    go(ag_own(0, 1))
    go(ag_own(1, 0))

    def qrows(q, i):
        return pl.ds(pl.multiple_of(q * QD + QOFF[i], 16), QROWS[i])

    def qcols(q, i):
        w = CWS[i] // 4
        return pl.ds(pl.multiple_of(COFF[i] + q * w, w), w)

    def region(m, g, core, q, i):
        r = qrows(q, i) if m < 2 else None
        if m == 0:
            return wq_v.at[g, core, r, :]
        if m == 1:
            return wkv_v.at[g, r, pl.ds(pl.multiple_of(core * HD, HD), HD)]
        return wo_v.at[
            pl.ds(pl.multiple_of((g * 2 + core) * 256, 256), 256),
            qcols(q, i),
        ]

    def own_region(m, q, i):
        if m == 0:
            return wq.at[qrows(q, i), :]
        if m == 1:
            return wkv.at[qrows(q, i), :]
        return wo.at[:, qcols(q, i)]

    def parts(s):
        return [(0, s), (1, s)] if s < NQ else [(2, s - NQ)]

    def sem_ix(m, i):
        return m * NQ + i

    q_cc = 2 * xl + b
    q_x = 2 * (1 - xl) + b
    q_zc = 2 * xl + 1 - b
    q_zx = 2 * (1 - xl) + 1 - b

    def cross_send(s):
        for m, i in parts(s):
            k = sem_ix(m, i)
            go(remote(own_region(m, q_x, i), region(m, 1, c, q_x, i),
                      w_s.at[0, k], w_r.at[0, k], cross))

    def across_send(s):
        for m, i in parts(s):
            k = sem_ix(m, i)
            go(remote(own_region(m, q_zc, i), region(m, 1, c, q_zc, i),
                      w_s.at[3, k], w_r.at[3, k], cross))

    def w_wait(ch, m, core, q, i):
        k = sem_ix(m, i)
        reg = region(m, 1, core, q, i)
        remote(reg, reg, w_s.at[ch, k], w_r.at[ch, k], part).wait_recv()

    def w_send(ch, m, q, i, dev):
        k = sem_ix(m, i)
        reg = region(m, 1, c, q, i)
        go(remote(reg, reg, w_s.at[ch, k], w_r.at[ch, k], dev))

    def ev_cross(s):
        z_dev = (zp, zm)[s % 2]
        for m, i in parts(s):
            w_wait(0, m, c, q_cc, i)
            w_send(1, m, q_cc, i, xlo)
            w_send(2, m, q_cc, i, z_dev)
            w_send(4, m, q_cc, i, part)

    def ev_xlo(s):
        z_dev = (zp, zm)[s % 2]
        for m, i in parts(s):
            w_wait(1, m, c, q_x, i)
            if s < DIRECT:
                w_send(3, m, q_x, i, z_dev)
            w_send(5, m, q_x, i, part)

    def ev_zc(s):
        for m, i in parts(s):
            w_wait(2, m, c, q_zc, i)
            w_send(6, m, q_zc, i, part)

    def ev_zx(s):
        for m, i in parts(s):
            w_wait(3, m, c, q_zx, i)
            w_send(7, m, q_zx, i, part)

    def part_wait(steps):
        for s in steps:
            for m, i in parts(s):
                for ch, q in ((4, q_cc), (5, q_x), (6, q_zc), (7, q_zx)):
                    w_wait(ch, m, 1 - c, q, i)

    def own_dst(m, core):
        return (
            wq_v.at[0, core],
            wkv_v.at[0, :, pl.ds(pl.multiple_of(core * HD, HD), HD)],
            wo_v.at[pl.ds(pl.multiple_of(core * 256, 256), 256), :],
        )[m]

    def own_to_part(m):
        go(remote((wq, wkv, wo)[m], own_dst(m, c), po_s.at[m], po_r.at[m], part))

    def own_part_wait(m):
        dst = own_dst(m, 1 - c)
        remote(dst, dst, po_s.at[m], po_r.at[m], part).wait_recv()

    def norm(slot, half):
        @pl.loop(0, HALF // 16)
        def _(r):
            r0 = pl.multiple_of(half * HALF + r * 16, 16)
            wide = hbuf[slot, pl.ds(r0, 16), :].astype(F32)
            ms = jnp.mean(wide * wide, axis=-1, keepdims=True)
            xn[pl.ds(pl.multiple_of(slot * SEQ + r0, 16), 16), :] = (
                wide * lax.rsqrt(ms + EPS) * gain_v[...]
            ).astype(BF)

    def rope(v):
        return v * tab_v[0] + pltpu.roll(v, HD // 2, 1) * tab_v[1]

    def attend(slot, g, kv, q0, q1):
        keys = rope(kv[:, :HD].astype(F32)).astype(BF)
        vals = kv[:, HD:]
        qs = jnp.concatenate(
            [rope(v).astype(BF) for v in (q0[:, :HD], q0[:, HD:], q1[:, :HD], q1[:, HD:])],
            axis=0,
        )
        sc = lax.dot_general(
            qs, keys, (((1,), (1,)), ((), ())), preferred_element_type=F32
        ) * (1.0 / math.sqrt(HD))
        rowi = lax.broadcasted_iota(jnp.int32, sc.shape, 0) % SEQ
        coli = lax.broadcasted_iota(jnp.int32, sc.shape, 1)
        sc = jnp.where(rowi >= coli, sc, -1e30)
        e = jnp.exp(sc - jnp.max(sc, axis=-1, keepdims=True))
        p = (e / jnp.sum(e, axis=-1, keepdims=True)).astype(BF)
        o = jnp.dot(p, vals, preferred_element_type=F32).astype(BF)
        for j in range(4):
            mx[slot, :, pl.ds(g * 512 + j * HD, HD)] = o[j * SEQ:(j + 1) * SEQ]

    def project(x, g, ks):
        def chain(w, some):
            v = None
            for k0, kn in some:
                d = jnp.dot(x(k0, kn), w[pl.ds(k0, kn), :], preferred_element_type=F32)
                v = d if v is None else v + d
            return v

        h = len(ks) // 2
        q0 = chain(wq_v.at[g, 0], ks)
        q1 = chain(wq_v.at[g, 1], ks)
        kv = chain(wkv_v.at[g], ks[:h]) + chain(wkv_v.at[g], ks[h:])
        return kv, q0, q1

    ALL_K = [(0, D // 2), (D // 2, D // 2)]

    def group_k(j):
        _, _, k0, kn = GROUPS[j]
        return [(q * QD + k0, kn) for q in range(4)]

    def attn(slot, g):
        kv, q0, q1 = project(
            lambda k0, kn: xn[pl.ds(slot * SEQ, SEQ), pl.ds(k0, kn)], g, ALL_K
        )
        attend(slot, g, kv.astype(BF), q0, q1)

    SETS = (((1, 0), (2, 1)), ((1, 1), (2, 0)))

    def proj_set(n, g, j):
        def x(k0, kn):
            return jnp.concatenate(
                [xn[pl.ds(sl * SEQ + hf * HALF, HALF), pl.ds(k0, kn)] for sl, hf in SETS[n]],
                axis=0,
            )

        for m, v in enumerate(project(x, g, ALL_K if j is None else group_k(j))):
            for u, (sl, hf) in enumerate(SETS[n]):
                pacc[g, m, pl.ds((sl - 1) * SEQ + hf * HALF, HALF), :] = v[
                    u * HALF:(u + 1) * HALF
                ]

    def proj_both(g, j):
        vs = project(
            lambda k0, kn: xn[pl.ds(SEQ, 2 * SEQ), pl.ds(k0, kn)], g, group_k(j)
        )
        vs = [pacc[g, m] + v for m, v in enumerate(vs)]
        if j < 2:
            for m, v in enumerate(vs):
                pacc[g, m] = v
        else:
            attend_both(g, vs)

    def attend_both(g, vs=None):
        for u in (1, 0):
            r = pl.ds(u * SEQ, SEQ)
            kv, q0, q1 = [
                pacc[g, m, r] if vs is None else vs[m][u * SEQ:(u + 1) * SEQ]
                for m in range(3)
            ]
            attend(1 + u, g, kv.astype(BF), q0, q1)

    def outp(slot, i):
        cols = pl.ds(COFF[i], CWS[i])
        o = jnp.dot(mx[slot], wo_v[:, cols], preferred_element_type=F32)
        if slot == 0:
            acc[:, cols] = o
        elif slot == 1:
            sbuf[0, pl.ds(0, HALF), cols] = o[:HALF].astype(BF)
            comb[1, :, cols] = o[HALF:]
        elif slot == 2:
            sbuf[1, pl.ds(HALF, HALF), cols] = o[HALF:].astype(BF)
            comb[0, :, cols] = o[:HALF]
        else:
            sbuf[2, :, cols] = o.astype(BF)

    def blk(ref, half, i):
        return ref.at[pl.ds(half * HALF, HALF), pl.ds(COFF[i], CWS[i])]

    def y_copy(direction, k, src, dst):
        return remote(src, dst, rs_s.at[direction, k], rs_r.at[direction, k],
                      right if direction == 0 else left)

    def rs_only(d, i):
        return y_copy(d, i, blk(sbuf.at[1 - d], 1 - d, i), blk(rf.at[d], 1 - d, i))

    def rs_diag(d, i):
        return y_copy(d, NC + i, blk(sbuf.at[2], d, i), blk(rd.at[d], 0, i))

    def rs_comb(d, i):
        return y_copy(d, 2 * NC + i, blk(sbuf.at[1 - d], d, i), blk(rf.at[d], d, i))

    def combine(d, i):
        rs_diag(d, i).wait_recv()
        cols = pl.ds(COFF[i], CWS[i])
        v = comb[d, :, cols] + rd[d, :, cols].astype(F32)
        sbuf[1 - d, pl.ds(d * HALF, HALF), cols] = v.astype(BF)
        go(rs_comb(d, i))

    outs = []

    def finish(half, i):
        rs_only(1 - half, i).wait_recv()
        rs_comb(half, i).wait_recv()
        rr, cols = pl.ds(half * HALF, HALF), pl.ds(COFF[i], CWS[i])
        v = acc[rr, cols] + rf[0, rr, cols].astype(F32) + rf[1, rr, cols].astype(F32)
        ob[rr, cols] = v.astype(BF)
        cp = pltpu.make_async_copy(
            ob.at[rr, cols], out.at[0, rr, cols], sem_o.at[half, i]
        )
        cp.start()
        outs.append(cp)

    plan = []

    def due(time, fn, *args):
        plan.append((time, len(plan), fn, args))

    def loaded(*ks):
        for k in ks:
            loads[k].wait()

    def ag_first():
        ag_wait(1, 0)
        go(ag_fwd(0))
        ag_wait(2, 1)
        go(ag_fwd(1))

    def outp_send(i):
        part_wait([NQ + i])
        outp(2, i)
        go(rs_only(0, i))
        outp(1, i)
        go(rs_only(1, i))

    def outp_diag(i):
        outp(3, i)
        go(rs_diag(0, i))
        go(rs_diag(1, i))

    t_c, t_x, t_zc, t_zx = arrivals(5.0)
    landed = [max(ts) + 2 for ts in zip(t_c, t_x, t_zc, t_zx)]
    last_qkv = max(landed[:NQ])
    written = []
    for s in range(NSTEP):
        for time, ev in ((t_c, ev_cross), (t_x, ev_xlo), (t_zc, ev_zc), (t_zx, ev_zx)):
            if time[s] < last_qkv:
                due(time[s], ev, s)
            else:
                written.append((ev, s))
    due(4.5, loaded, 0, 1)
    due(4.5, norm, 0, 0)
    due(4.5, norm, 0, 1)
    due(11.3, loaded, 2, 3, 4)
    due(11.3, own_part_wait, 0)
    due(11.3, own_part_wait, 1)
    due(11.3, attn, 0, 0)
    due(11.4, own_to_part, 2)
    due(18.5, ag_first)
    due(18.5, norm, 1, 0)
    due(18.5, norm, 2, 1)
    due(19.5, proj_set, 0, 0, None)
    due(30, ag_wait, 1, 1)
    due(30, norm, 1, 1)
    due(30, ag_wait, 2, 0)
    due(30, norm, 2, 0)
    due(30.5, proj_set, 1, 0, None)
    for j, (i0, n, _, _) in enumerate(GROUPS):
        when = max(landed[i0:i0 + n])
        if j == 2:
            due(when, attend_both, 0)
        due(when, part_wait, range(i0, i0 + n))
        if j == 0:
            due(when, proj_set, 0, 1, 0)
            due(max(when, 31.5), proj_set, 1, 1, 0)
        else:
            due(max(when, 32.6), proj_both, 1, j)

    def then(fn, *args):
        due(last_qkv + 1, fn, *args)

    def relays(upto):
        for ev in (ev_cross, ev_xlo, ev_zc, ev_zx):
            for w in [w for w in written if w[0] is ev and w[1] <= NQ + upto]:
                then(*w)
                written.remove(w)

    then(loaded, 5)
    then(own_part_wait, 2)
    relays(0)
    then(outp_send, 0)
    for w in [w for w in written if w[0] is ev_cross]:
        then(*w)
        written.remove(w)
    relays(2)
    then(attn, 0, 1)
    then(outp_send, 1)
    then(outp_send, 2)
    relays(3)
    for half in (0, 1):
        then(ag_wait, 3, half)
        then(norm, 3, half)
    then(outp_send, 3)
    relays(5)
    then(attn, 3, 0)
    then(outp_send, 4)
    then(outp_send, 5)
    then(attn, 3, 1)
    for i in range(NC):
        then(outp_diag, i)
    for i in range(NC):
        then(outp, 0, i)
    for i in range(NC):
        then(combine, 0, i)
        then(combine, 1, i)
    for i in range(NC):
        then(finish, 0, i)
        then(finish, 1, i)

    assert not written
    for s in range(NSTEP):
        cross_send(s)
    for s in range(DIRECT, NSTEP):
        across_send(s)
    own_to_part(0)
    own_to_part(1)
    plan.sort(key=lambda p: p[:2])
    at = {(p[2], p[3]): k for k, p in enumerate(plan)}
    for i in range(NC):
        assert at[outp_send, (i,)] > max(at[ev_zx, (NQ + i,)], at[ev_zc, (NQ + i,)])
        assert at[outp_diag, (i,)] > at[outp_send, (i,)]
    for s in range(NSTEP):
        assert at[ev_cross, (s,)] < at[ev_xlo, (s,)] < at[ev_zx, (s,)]
        assert at[ev_cross, (s,)] < at[ev_zc, (s,)]
    for j, (i0, n, _, _) in enumerate(GROUPS):
        for s in range(i0, i0 + n):
            pj = (proj_both, (1, j)) if j else (proj_set, (0, 1, 0))
            assert at[pj] > max(at[ev_zx, (s,)], at[ev_zc, (s,)])
            assert at[part_wait, (range(i0, i0 + n),)] > max(at[ev_zx, (s,)], at[ev_zc, (s,)])
    for time, _, fn, args in plan:
        fn(*args)
    for cp in outs:
        cp.wait()
    for cp in sent:
        cp.wait_send()


def shards(hidden_in, norm_gain, query_weight, kv_weight, output_weight):
    tab = jnp.asarray(tables())
    anyspec = pl.BlockSpec(memory_space=pl.ANY)
    dma = pltpu.SemaphoreType.DMA
    return pl.pallas_call(
        kernel,
        out_shape=jax.ShapeDtypeStruct((1, SEQ, D), BF),
        in_specs=[anyspec] * 6,
        out_specs=anyspec,
        scratch_shapes=[
            pltpu.VMEM((4, SEQ, D), BF),
            pltpu.VMEM((4 * SEQ, D), BF),
            pltpu.VMEM((1, D), F32),
            pltpu.VMEM((2, SEQ, HD), F32),
            pltpu.VMEM((2, 2, D, 2 * HD), BF),
            pltpu.VMEM((2, D, 2 * HD), BF),
            pltpu.VMEM((1024, D), BF),
            pltpu.VMEM((4, SEQ, 1024), BF),
            pltpu.VMEM((2, 3, 2 * SEQ, 2 * HD), F32),
            pltpu.VMEM((SEQ, D), F32),
            pltpu.VMEM((2, HALF, D), F32),
            pltpu.VMEM((3, SEQ, D), BF),
            pltpu.VMEM((2, HALF, D), BF),
            pltpu.VMEM((2, SEQ, D), BF),
            pltpu.VMEM((SEQ, D), BF),
            dma((6,)),
            dma((2, NC)),
            dma((2, 3)),
            dma((4, 2)),
            dma((8, 2 * NQ + NC)),
            dma((8, 2 * NQ + NC)),
            dma((3,)),
            dma((3,)),
            dma((2, 3 * NC)),
            dma((2, 3 * NC)),
        ],
        compiler_params=pltpu.CompilerParams(
            collective_id=0, has_side_effects=True, vmem_limit_bytes=67000000
        ),
        cost_estimate=pl.CostEstimate(
            flops=11_000_000_000, bytes_accessed=8_000_000, transcendentals=600_000
        ),
    )(hidden_in, norm_gain.reshape(1, D), tab, query_weight, kv_weight, output_weight)


def solution(mesh):
    placed = (
        P(("dp", "tensor"), None, None),
        P(),
        P(None, "tensor"),
        P(None, "tensor"),
        P("tensor", None),
    )
    return jax.shard_map(
        shards,
        mesh=mesh,
        in_specs=placed,
        out_specs=P(("dp", "tensor"), None, None),
        check_vma=False,
    )
```

```python
import math

import jax
import jax.numpy as jnp
import numpy as np
from jax import lax
from jax.experimental import pallas as pl
from jax.experimental.pallas import tpu as pltpu
from jax.sharding import PartitionSpec as P

HD = 128
EPS = 1e-05
THETA = 500000.0
SEQ = 128
D = 4096
HALF = SEQ // 2
QROWS = (80, 80, 96, 128, 128, 96, 80, 80, 96, 96, 64)
QOFF = tuple(sum(QROWS[:i]) for i in range(len(QROWS)))
NQ = len(QROWS)
GROUPS = ((0, 5, 0, 512), (5, 3, 512, 256), (8, 3, 768, 256))
CWS = (512, 512, 1024, 1024, 512, 512)
COFF = tuple(sum(CWS[:i]) for i in range(len(CWS)))
NC = len(CWS)
NSTEP = NQ + NC
DIRECT = NQ + 2
QD = D // 4
BF = jnp.bfloat16
F32 = jnp.float32
MESH = pl.DeviceIdType.MESH


def tables():
    i = np.arange(HD // 2, dtype=np.float64)
    ang = np.arange(SEQ, dtype=np.float64)[:, None] * THETA ** (-2.0 * i / HD)[None, :]
    cos, sin = np.cos(ang), np.sin(ang)
    return np.stack(
        [np.concatenate([cos, cos], 1), np.concatenate([-sin, sin], 1)]
    ).astype(np.float32)


def arrivals(start):
    rate, hop = 46.6e3, 2.0
    size = [2 * r * 3 * HD for r in QROWS] + [2 * 2 * HD * w // 4 for w in CWS]
    wire = [b / rate for b in size]
    t_zc, t_zx = [0.0] * NSTEP, [0.0] * NSTEP
    t_c, free = [], start + 1.0
    for w in wire:
        free += w
        t_c.append(free + hop)
    for s in range(DIRECT, NSTEP):
        free += wire[s]
        t_zx[s] = free + hop
    t_x, free = [], 0.0
    for s, w in enumerate(wire):
        free = max(free, t_c[s]) + w
        t_x.append(free + hop)
    for side in (0, 1):
        jobs = [(t_c[s], 0, s) for s in range(side, NSTEP, 2)]
        jobs += [(t_x[s], 1, s) for s in range(side, DIRECT, 2)]
        free = 0.0
        for ready, kind, s in sorted(jobs):
            free = max(free, ready) + wire[s]
            (t_zc, t_zx)[kind][s] = free + hop
    return t_c, t_x, t_zc, t_zx


def kernel(
    h, gain, tab, wq, wkv, wo, out,
    hbuf, xn, gain_v, tab_v, wq_v, wkv_v, wo_v, mx, pacc,
    acc, comb, sbuf, rd, rf, ob,
    sem_l, sem_o, ag_s, ag_r, w_s, w_r, p_r, po_s, po_r, rs_s, rs_r,
):
    dp = lax.axis_index("dp")
    t = lax.axis_index("tensor")
    z, xl = dp // 2, dp % 2
    xh, y, c = t // 8, (t // 2) % 4, t % 2
    b = z % 2

    def at_y(yy):
        return (dp, xh * 8 + yy * 2 + c)

    right, left = at_y((y + 1) % 4), at_y((y + 3) % 4)
    cross = (z * 2 + 1 - xl, (1 - xh) * 8 + y * 2 + c)
    xlo = (z * 2 + 1 - xl, t)
    zp = (((z + 1) % 8) * 2 + xl, t)
    zm = (((z + 7) % 8) * 2 + xl, t)
    part = (dp, t + 1 - 2 * c)

    def remote(src, dst, ss, rs, dev):
        return pltpu.make_async_remote_copy(
            src_ref=src, dst_ref=dst, send_sem=ss, recv_sem=rs,
            device_id=dev, device_id_type=MESH,
        )

    loads = [
        pltpu.make_async_copy(h.at[0], hbuf.at[0], sem_l.at[0]),
        pltpu.make_async_copy(gain, gain_v, sem_l.at[1]),
        pltpu.make_async_copy(tab, tab_v, sem_l.at[2]),
        pltpu.make_async_copy(wq, wq_v.at[0, c], sem_l.at[3]),
        pltpu.make_async_copy(
            wkv, wkv_v.at[0, :, pl.ds(pl.multiple_of(c * HD, HD), HD)], sem_l.at[4]
        ),
        pltpu.make_async_copy(
            wo, wo_v.at[pl.ds(pl.multiple_of(c * 256, 256), 256), :], sem_l.at[5]
        ),
    ]
    for cp in loads:
        cp.start()

    barrier = pltpu.get_barrier_semaphore()
    for dev in (right, left, cross, xlo, zp, zm, part):
        pl.semaphore_signal(barrier, inc=1, device_id=dev, device_id_type=MESH)
    pl.semaphore_wait(barrier, 7)

    sent = []

    def go(cp):
        cp.start()
        sent.append(cp)

    def rows(ref, half):
        return ref.at[pl.ds(half * HALF, HALF), :]

    def ag_own(direction, half):
        dst = hbuf.at[1 if direction == 0 else 2]
        return remote(
            rows(h.at[0], half), rows(dst, half),
            ag_s.at[direction, half], ag_r.at[1 + direction, half],
            right if direction == 0 else left,
        )

    def ag_fwd(direction):
        half = direction
        return remote(
            rows(hbuf.at[1 + direction], half), rows(hbuf.at[3], half),
            ag_s.at[direction, 2], ag_r.at[3, half],
            right if direction == 0 else left,
        )

    def ag_wait(slot, half):
        remote(
            rows(hbuf.at[slot], half), rows(hbuf.at[slot], half),
            ag_s.at[0, 0], ag_r.at[slot, half], right,
        ).wait_recv()

    go(ag_own(0, 0))
    go(ag_own(1, 1))
    go(ag_own(0, 1))
    go(ag_own(1, 0))

    def qrows(q, i):
        return pl.ds(pl.multiple_of(q * QD + QOFF[i], 16), QROWS[i])

    def qcols(q, i):
        w = CWS[i] // 4
        return pl.ds(pl.multiple_of(COFF[i] + q * w, w), w)

    def region(m, g, core, q, i):
        r = qrows(q, i) if m < 2 else None
        if m == 0:
            return wq_v.at[g, core, r, :]
        if m == 1:
            return wkv_v.at[g, r, pl.ds(pl.multiple_of(core * HD, HD), HD)]
        return wo_v.at[
            pl.ds(pl.multiple_of((g * 2 + core) * 256, 256), 256),
            qcols(q, i),
        ]

    def own_region(m, q, i):
        if m == 0:
            return wq.at[qrows(q, i), :]
        if m == 1:
            return wkv.at[qrows(q, i), :]
        return wo.at[:, qcols(q, i)]

    def parts(s):
        return [(0, s), (1, s)] if s < NQ else [(2, s - NQ)]

    def sem_ix(m, i):
        return m * NQ + i

    q_cc = 2 * xl + b
    q_x = 2 * (1 - xl) + b
    q_zc = 2 * xl + 1 - b
    q_zx = 2 * (1 - xl) + 1 - b

    def cross_send(s):
        for m, i in parts(s):
            k = sem_ix(m, i)
            remote(own_region(m, q_x, i), region(m, 1, c, q_x, i),
                   w_s.at[0, m], w_r.at[0, k], cross).start()

    def across_send(s):
        for m, i in parts(s):
            k = sem_ix(m, i)
            remote(own_region(m, q_zc, i), region(m, 1, c, q_zc, i),
                   w_s.at[3, m], w_r.at[3, k], cross).start()

    def w_wait(ch, m, core, q, i):
        k = sem_ix(m, i)
        reg = region(m, 1, core, q, i)
        remote(reg, reg, w_s.at[ch, m], w_r.at[ch, k], part).wait_recv()

    def w_send(ch, m, q, i, dev):
        reg = region(m, 1, c, q, i)
        if ch < 4:
            got = w_r.at[ch, sem_ix(m, i)]
        elif m < 2:
            got = p_r.at[m * 3 + sum(i >= g[0] for g in GROUPS[1:])]
        else:
            got = p_r.at[6 + i]
        remote(reg, reg, w_s.at[min(ch, 4), m], got, dev).start()

    def ev_cross(s):
        z_dev = (zp, zm)[s % 2]
        for m, i in parts(s):
            w_wait(0, m, c, q_cc, i)
            w_send(1, m, q_cc, i, xlo)
            w_send(2, m, q_cc, i, z_dev)
            w_send(4, m, q_cc, i, part)

    def ev_xlo(s):
        z_dev = (zp, zm)[s % 2]
        for m, i in parts(s):
            w_wait(1, m, c, q_x, i)
            if s < DIRECT:
                w_send(3, m, q_x, i, z_dev)
            w_send(5, m, q_x, i, part)

    def ev_zc(s):
        for m, i in parts(s):
            w_wait(2, m, c, q_zc, i)
            w_send(6, m, q_zc, i, part)

    def ev_zx(s):
        for m, i in parts(s):
            w_wait(3, m, c, q_zx, i)
            w_send(7, m, q_zx, i, part)

    def some(m, core, rows, cols):
        if m == 0:
            return wq_v.at[1, core, pl.ds(0, rows), :]
        if m == 1:
            return wkv_v.at[1, pl.ds(0, rows), pl.ds(pl.multiple_of(core * HD, HD), HD)]
        return wo_v.at[pl.ds(pl.multiple_of((2 + core) * 256, 256), 256), cols]

    def part_wait(steps):
        s0 = steps[0]
        for m in (0, 1) if s0 < NQ else (2,):
            if m < 2:
                reg = some(m, 1 - c, 4 * sum(QROWS[s] for s in steps), None)
                got = p_r.at[m * 3 + sum(s0 >= g[0] for g in GROUPS[1:])]
            else:
                reg = some(2, 1 - c, None, pl.ds(COFF[s0 - NQ], CWS[s0 - NQ]))
                got = p_r.at[6 + s0 - NQ]
            remote(reg, reg, w_s.at[4, m], got, part).wait_recv()

    def weights_sent():
        for kind in range(5):
            for m in range(3):
                n = D if kind == 4 else QD
                reg = some(m, c, n, pl.ds(0, n))
                remote(reg, reg, w_s.at[kind, m], w_r.at[0, 0], part).wait_send()

    def own_dst(m, core):
        return (
            wq_v.at[0, core],
            wkv_v.at[0, :, pl.ds(pl.multiple_of(core * HD, HD), HD)],
            wo_v.at[pl.ds(pl.multiple_of(core * 256, 256), 256), :],
        )[m]

    def own_to_part(m):
        go(remote((wq, wkv, wo)[m], own_dst(m, c), po_s.at[m], po_r.at[m], part))

    def own_part_wait(m):
        dst = own_dst(m, 1 - c)
        remote(dst, dst, po_s.at[m], po_r.at[m], part).wait_recv()

    def norm(slot, half):
        @pl.loop(0, HALF // 16)
        def _(r):
            r0 = pl.multiple_of(half * HALF + r * 16, 16)
            wide = hbuf[slot, pl.ds(r0, 16), :].astype(F32)
            ms = jnp.mean(wide * wide, axis=-1, keepdims=True)
            xn[pl.ds(pl.multiple_of(slot * SEQ + r0, 16), 16), :] = (
                wide * lax.rsqrt(ms + EPS) * gain_v[...]
            ).astype(BF)

    def rope(v):
        return v * tab_v[0] + pltpu.roll(v, HD // 2, 1) * tab_v[1]

    def attend(slot, g, kv, q0, q1):
        keys = rope(kv[:, :HD].astype(F32)).astype(BF)
        vals = kv[:, HD:]
        qs = jnp.concatenate(
            [rope(v).astype(BF) for v in (q0[:, :HD], q0[:, HD:], q1[:, :HD], q1[:, HD:])],
            axis=0,
        )
        sc = lax.dot_general(
            qs, keys, (((1,), (1,)), ((), ())), preferred_element_type=F32
        ) * (1.0 / math.sqrt(HD))
        rowi = lax.broadcasted_iota(jnp.int32, sc.shape, 0) % SEQ
        coli = lax.broadcasted_iota(jnp.int32, sc.shape, 1)
        sc = jnp.where(rowi >= coli, sc, -1e30)
        e = jnp.exp(sc - jnp.max(sc, axis=-1, keepdims=True))
        p = (e / jnp.sum(e, axis=-1, keepdims=True)).astype(BF)
        o = jnp.dot(p, vals, preferred_element_type=F32).astype(BF)
        for j in range(4):
            mx[slot, :, pl.ds(g * 512 + j * HD, HD)] = o[j * SEQ:(j + 1) * SEQ]

    def project(x, g, ks):
        def chain(w, some):
            v = None
            for k0, kn in some:
                d = jnp.dot(x(k0, kn), w[pl.ds(k0, kn), :], preferred_element_type=F32)
                v = d if v is None else v + d
            return v

        h = len(ks) // 2
        q0 = chain(wq_v.at[g, 0], ks)
        q1 = chain(wq_v.at[g, 1], ks)
        kv = chain(wkv_v.at[g], ks[:h]) + chain(wkv_v.at[g], ks[h:])
        return kv, q0, q1

    ALL_K = [(0, D // 2), (D // 2, D // 2)]

    def group_k(j):
        _, _, k0, kn = GROUPS[j]
        return [(q * QD + k0, kn) for q in range(4)]

    def attn(slot, g):
        kv, q0, q1 = project(
            lambda k0, kn: xn[pl.ds(slot * SEQ, SEQ), pl.ds(k0, kn)], g, ALL_K
        )
        attend(slot, g, kv.astype(BF), q0, q1)

    SETS = (((1, 0), (2, 1)), ((1, 1), (2, 0)))

    def proj_set(n, g, j):
        def x(k0, kn):
            return jnp.concatenate(
                [xn[pl.ds(sl * SEQ + hf * HALF, HALF), pl.ds(k0, kn)] for sl, hf in SETS[n]],
                axis=0,
            )

        for m, v in enumerate(project(x, g, ALL_K if j is None else group_k(j))):
            for u, (sl, hf) in enumerate(SETS[n]):
                pacc[g, m, pl.ds((sl - 1) * SEQ + hf * HALF, HALF), :] = v[
                    u * HALF:(u + 1) * HALF
                ]

    def proj_both(g, j):
        vs = project(
            lambda k0, kn: xn[pl.ds(SEQ, 2 * SEQ), pl.ds(k0, kn)], g, group_k(j)
        )
        vs = [pacc[g, m] + v for m, v in enumerate(vs)]
        if j < 2:
            for m, v in enumerate(vs):
                pacc[g, m] = v
        else:
            attend_both(g, vs)

    def attend_both(g, vs=None):
        for u in (1, 0):
            r = pl.ds(u * SEQ, SEQ)
            kv, q0, q1 = [
                pacc[g, m, r] if vs is None else vs[m][u * SEQ:(u + 1) * SEQ]
                for m in range(3)
            ]
            attend(1 + u, g, kv.astype(BF), q0, q1)

    def outp(slot, i):
        cols = pl.ds(COFF[i], CWS[i])
        o = jnp.dot(mx[slot], wo_v[:, cols], preferred_element_type=F32)
        if slot == 0:
            acc[:, cols] = o
        elif slot == 1:
            sbuf[0, pl.ds(0, HALF), cols] = o[:HALF].astype(BF)
            comb[1, :, cols] = o[HALF:]
        elif slot == 2:
            sbuf[1, pl.ds(HALF, HALF), cols] = o[HALF:].astype(BF)
            comb[0, :, cols] = o[:HALF]
        else:
            sbuf[2, :, cols] = o.astype(BF)

    def blk(ref, half, i):
        return ref.at[pl.ds(half * HALF, HALF), pl.ds(COFF[i], CWS[i])]

    def y_copy(direction, k, src, dst):
        return remote(src, dst, rs_s.at[direction, k], rs_r.at[direction, k],
                      right if direction == 0 else left)

    def rs_only(d, i):
        return y_copy(d, i, blk(sbuf.at[1 - d], 1 - d, i), blk(rf.at[d], 1 - d, i))

    def rs_diag(d, i):
        return y_copy(d, NC + i, blk(sbuf.at[2], d, i), blk(rd.at[d], 0, i))

    def rs_comb(d, i):
        return y_copy(d, 2 * NC + i, blk(sbuf.at[1 - d], d, i), blk(rf.at[d], d, i))

    def combine(d, i):
        rs_diag(d, i).wait_recv()
        cols = pl.ds(COFF[i], CWS[i])
        v = comb[d, :, cols] + rd[d, :, cols].astype(F32)
        sbuf[1 - d, pl.ds(d * HALF, HALF), cols] = v.astype(BF)
        go(rs_comb(d, i))

    outs = []

    def finish(half, i):
        rs_only(1 - half, i).wait_recv()
        rs_comb(half, i).wait_recv()
        rr, cols = pl.ds(half * HALF, HALF), pl.ds(COFF[i], CWS[i])
        v = acc[rr, cols] + rf[0, rr, cols].astype(F32) + rf[1, rr, cols].astype(F32)
        ob[rr, cols] = v.astype(BF)
        cp = pltpu.make_async_copy(
            ob.at[rr, cols], out.at[0, rr, cols], sem_o.at[half, i]
        )
        cp.start()
        outs.append(cp)

    plan = []

    def due(time, fn, *args):
        plan.append((time, len(plan), fn, args))

    def loaded(*ks):
        for k in ks:
            loads[k].wait()

    def ag_first():
        ag_wait(1, 0)
        go(ag_fwd(0))
        ag_wait(2, 1)
        go(ag_fwd(1))

    def outp_send(i):
        part_wait([NQ + i])
        outp(2, i)
        go(rs_only(0, i))
        outp(1, i)
        go(rs_only(1, i))

    def outp_diag(i):
        outp(3, i)
        go(rs_diag(0, i))
        go(rs_diag(1, i))

    t_c, t_x, t_zc, t_zx = arrivals(5.0)
    landed = [max(ts) + 2 for ts in zip(t_c, t_x, t_zc, t_zx)]
    last_qkv = max(landed[:NQ])
    written = []
    for s in range(NSTEP):
        for time, ev in ((t_c, ev_cross), (t_x, ev_xlo), (t_zc, ev_zc), (t_zx, ev_zx)):
            if time[s] < last_qkv:
                due(time[s], ev, s)
            else:
                written.append((ev, s))
    due(4.5, loaded, 0, 1)
    due(4.5, norm, 0, 0)
    due(4.5, norm, 0, 1)
    due(11.3, loaded, 2, 3, 4)
    due(11.3, own_part_wait, 0)
    due(11.3, own_part_wait, 1)
    due(11.3, attn, 0, 0)
    due(11.4, own_to_part, 2)
    due(18.5, ag_first)
    due(18.5, norm, 1, 0)
    due(18.5, norm, 2, 1)
    due(19.5, proj_set, 0, 0, None)
    due(30, ag_wait, 1, 1)
    due(30, norm, 1, 1)
    due(30, ag_wait, 2, 0)
    due(30, norm, 2, 0)
    due(30.5, proj_set, 1, 0, None)
    for j, (i0, n, _, _) in enumerate(GROUPS):
        when = max(landed[i0:i0 + n])
        if j == 2:
            due(when, attend_both, 0)
        due(when, part_wait, range(i0, i0 + n))
        if j == 0:
            due(when, proj_set, 0, 1, 0)
            due(max(when, 31.5), proj_set, 1, 1, 0)
        else:
            due(max(when, 32.6), proj_both, 1, j)

    def then(fn, *args):
        due(last_qkv + 1, fn, *args)

    def relays(upto):
        for ev in (ev_cross, ev_xlo, ev_zc, ev_zx):
            for w in [w for w in written if w[0] is ev and w[1] <= NQ + upto]:
                then(*w)
                written.remove(w)

    then(loaded, 5)
    then(own_part_wait, 2)
    relays(0)
    then(outp_send, 0)
    for w in [w for w in written if w[0] is ev_cross]:
        then(*w)
        written.remove(w)
    relays(2)
    then(attn, 0, 1)
    then(outp_send, 1)
    then(outp_send, 2)
    relays(3)
    for half in (0, 1):
        then(ag_wait, 3, half)
        then(norm, 3, half)
    then(outp_send, 3)
    relays(5)
    then(attn, 3, 0)
    then(outp_send, 4)
    then(outp_send, 5)
    then(attn, 3, 1)
    for i in range(NC):
        then(outp_diag, i)
    for i in range(NC):
        then(outp, 0, i)
    for i in range(NC):
        then(combine, 0, i)
        then(combine, 1, i)
    for i in range(NC):
        then(finish, 0, i)
        then(finish, 1, i)

    assert not written
    for s in range(NSTEP):
        cross_send(s)
    for s in range(DIRECT, NSTEP):
        across_send(s)
    own_to_part(0)
    own_to_part(1)
    plan.sort(key=lambda p: p[:2])
    at = {(p[2], p[3]): k for k, p in enumerate(plan)}
    for i in range(NC):
        assert at[outp_send, (i,)] > max(at[ev_zx, (NQ + i,)], at[ev_zc, (NQ + i,)])
        assert at[outp_diag, (i,)] > at[outp_send, (i,)]
    for s in range(NSTEP):
        assert at[ev_cross, (s,)] < at[ev_xlo, (s,)] < at[ev_zx, (s,)]
        assert at[ev_cross, (s,)] < at[ev_zc, (s,)]
    for j, (i0, n, _, _) in enumerate(GROUPS):
        for s in range(i0, i0 + n):
            pj = (proj_both, (1, j)) if j else (proj_set, (0, 1, 0))
            assert at[pj] > max(at[ev_zx, (s,)], at[ev_zc, (s,)])
            assert at[part_wait, (range(i0, i0 + n),)] > max(at[ev_zx, (s,)], at[ev_zc, (s,)])
    for time, _, fn, args in plan:
        fn(*args)
    for cp in outs:
        cp.wait()
    for cp in sent:
        cp.wait_send()
    weights_sent()


def shards(hidden_in, norm_gain, query_weight, kv_weight, output_weight):
    tab = jnp.asarray(tables())
    anyspec = pl.BlockSpec(memory_space=pl.ANY)
    dma = pltpu.SemaphoreType.DMA
    return pl.pallas_call(
        kernel,
        out_shape=jax.ShapeDtypeStruct((1, SEQ, D), BF),
        in_specs=[anyspec] * 6,
        out_specs=anyspec,
        scratch_shapes=[
            pltpu.VMEM((4, SEQ, D), BF),
            pltpu.VMEM((4 * SEQ, D), BF),
            pltpu.VMEM((1, D), F32),
            pltpu.VMEM((2, SEQ, HD), F32),
            pltpu.VMEM((2, 2, D, 2 * HD), BF),
            pltpu.VMEM((2, D, 2 * HD), BF),
            pltpu.VMEM((1024, D), BF),
            pltpu.VMEM((4, SEQ, 1024), BF),
            pltpu.VMEM((2, 3, 2 * SEQ, 2 * HD), F32),
            pltpu.VMEM((SEQ, D), F32),
            pltpu.VMEM((2, HALF, D), F32),
            pltpu.VMEM((3, SEQ, D), BF),
            pltpu.VMEM((2, HALF, D), BF),
            pltpu.VMEM((2, SEQ, D), BF),
            pltpu.VMEM((SEQ, D), BF),
            dma((6,)),
            dma((2, NC)),
            dma((2, 3)),
            dma((4, 2)),
            dma((5, 3)),
            dma((4, 2 * NQ + NC)),
            dma((6 + NC,)),
            dma((3,)),
            dma((3,)),
            dma((2, 3 * NC)),
            dma((2, 3 * NC)),
        ],
        compiler_params=pltpu.CompilerParams(
            collective_id=0, has_side_effects=True, vmem_limit_bytes=67000000
        ),
        cost_estimate=pl.CostEstimate(
            flops=11_000_000_000, bytes_accessed=8_000_000, transcendentals=600_000
        ),
    )(hidden_in, norm_gain.reshape(1, D), tab, query_weight, kv_weight, output_weight)


def solution(mesh):
    placed = (
        P(("dp", "tensor"), None, None),
        P(),
        P(None, "tensor"),
        P(None, "tensor"),
        P("tensor", None),
    )
    return jax.shard_map(
        shards,
        mesh=mesh,
        in_specs=placed,
        out_specs=P(("dp", "tensor"), None, None),
        check_vma=False,
    )
```
